32 devices in a mesh: gz: 2 (over x), gx: 2 (over core), gy: 8 (over z, y).
Axes of the slice: x: 2, y: 2, z: 4, core: 2. Of those that a mesh axis runs over, the one named last changes fastest.
Arguments:
- initial_field: float32 [128, 16, 1024], P('gz', 'gx', 'gy'), may hold values from -36 to 36
- plane_coupling: float32 [128, 16, 1024], P('gz', 'gx', 'gy'), may hold values from 0.06 to 0.24
- line_coupling: float32 [128, 16, 1024], P('gz', 'gx', 'gy'), may hold values from 1000 to 8000
- source: float32 [128, 16, 1024], P('gz', 'gx', 'gy'), may hold values from -4 to 4, as said below
- shift_table: float32 [8], replicated, may hold values from 0.5 to 1
- shift_index: int32 [4], replicated, may hold values from 0 to 7
Outputs:
- heated: float32 [128, 16, 1024], P('gz', 'gx', 'gy')
The draws below stay inside these ranges and needn't reach their ends.
Inputs may be any that keep to these rules, and one draw needn't show every extreme that they name: `shift_index`: one table row for each half-step. A heat source.
All inputs are finite; a program needn't handle non-finite values.
Results may differ from the reference program's by a relative error of at most 0.0003.
Values sent between devices are 32-bit elements; how exact they have to be, the bound alone decides.
A program may use at most 64 MiB of HBM per device.

```python
import math
import jax
import jax.numpy as jnp
from jax import lax

SHIFTS = 8
HALF = 4
NX = 16
NY = 1024
NZ = 128


def draw_source(key, part):
    values = jnp.clip(jax.random.normal(key, (NZ, NX, NY), jnp.float32), -4.0, 4.0)
    return values


def place_ends(entries, rng, least, top_value):
    dims = entries.shape
    place = [jax.random.randint(jax.random.fold_in(rng, axis), (), 0, dims[axis]) for axis in range(len(dims))]
    entries = entries.at[tuple(place)].set(least)
    longest = dims.index(max(dims))
    place[longest] = (place[longest] + 1) % dims[longest]
    return entries.at[tuple(place)].set(top_value)


def block_scale(stream_key, dims, shards, low, top_value):
    level = 1.0
    for axis_at, blocks in shards:
        draws = jax.random.uniform(jax.random.fold_in(jax.random.fold_in(stream_key, 6), axis_at), (blocks,), jnp.float32, low / len(shards), top_value / len(shards))
        level = level * jnp.repeat(jnp.exp(draws), dims[axis_at] // blocks).reshape((-1,) + (1,) * (len(dims) - 1 - axis_at))
    return level


def centred(stream_key, dims, scale, most, shards=(), kind=jnp.bfloat16):
    loudness = block_scale(stream_key, dims, shards, -0.22, 0.18) if shards else 1.0
    array = jax.random.normal(stream_key, dims, jnp.float32) * scale * loudness
    return jnp.minimum(jnp.maximum(array, -most), most).astype(kind)


def setup_inputs(seed: int = 0) -> dict:
    seeds = jax.random.split(jax.random.key(seed), 7)
    initial_field = centred(seeds[0], (NZ, NX, NY), 6.0, 36.0, ((0, 2), (1, 2), (2, 8)), jnp.float32)
    plane_coupling = jnp.clip(jnp.exp(math.log(0.24) - 1.3862944 * jax.random.uniform(seeds[1], (NZ, NX, NY), jnp.float32) ** block_scale(seeds[1], (NZ, NX, NY), ((0, 2), (1, 2), (2, 8)), -0.2, 0.2)), 0.06, 0.24)
    line_coupling = jnp.clip(jnp.exp(math.log(8000.0) - 2.0794415 * jax.random.uniform(seeds[2], (NZ, NX, NY), jnp.float32) ** block_scale(seeds[2], (NZ, NX, NY), ((0, 2), (1, 2), (2, 8)), -0.2, 0.2)), 1000.0, 8000.0)
    source = draw_source(jax.random.fold_in(seeds[6], 71), 0)
    shift_table = jnp.clip(jax.random.uniform(seeds[4], (SHIFTS,), jnp.float32, 0.5, 1.0), 0.5, 1.0)
    shift_index = place_ends(jax.random.randint(seeds[5], (HALF,), 0, SHIFTS), jax.random.fold_in(seeds[5], 1), 0, SHIFTS - 1).astype(jnp.int32)
    return {"initial_field": initial_field, "plane_coupling": plane_coupling, "line_coupling": line_coupling, "source": source, "shift_table": shift_table, "shift_index": shift_index}


def lookup(shift_table, table_row):
    table_slots = jnp.arange(shift_table.shape[0], dtype=jnp.int32)
    return jnp.sum(jnp.where(table_slots == table_row, shift_table, jnp.zeros_like(shift_table)))


def plane_apply(current, coupling):
    padded = jnp.pad(current, ((0, 0), (1, 1), (1, 1)))
    beside_all = padded[:, 2:, 1:-1] + padded[:, :-2, 1:-1] + padded[:, 1:-1, 2:] + padded[:, 1:-1, :-2]
    return coupling * (beside_all - 4.0 * current)


def line_solve(explicit, line_coupling, shift_value):
    scaled = shift_value * line_coupling
    center = 1.0 + 2.0 * scaled

    def forward(previous, inputs):
        before_c, before_d = previous
        coupling, middle, right_side = inputs
        pivot_value = middle + coupling * before_c
        next_c = -coupling / pivot_value
        next_d = (right_side + coupling * before_d) / pivot_value
        return (next_c, next_d), (next_c, next_d)

    zero_plane = jnp.zeros_like(explicit[0])
    final_state, factors = lax.scan(forward, (zero_plane, zero_plane), (scaled, center, explicit))

    def backward(later_value, inputs):
        ratio, offset = inputs
        own_value = offset - ratio * later_value
        return own_value, own_value

    final_value, solved = lax.scan(backward, zero_plane, factors, reverse=True)
    return solved


def reference(initial_field, plane_coupling, line_coupling, source, shift_table, shift_index):
    current = initial_field
    for half_step in range(HALF):
        shift_value = lookup(shift_table, shift_index[half_step])
        explicit = current + shift_value * (plane_apply(current, plane_coupling) + source)
        current = line_solve(explicit, line_coupling, shift_value)
    return current
```

```python
import functools

import jax
import jax.numpy as jnp
from jax import lax
from jax.experimental import pallas as pl
from jax.experimental.pallas import tpu as pltpu
from jax.sharding import PartitionSpec as P


def loop(count, body, init, unroll, reverse=False):
    while count % unroll:
        unroll -= 1

    def block(i, carry):
        for j in range(unroll):
            k = i * unroll + j
            carry = body(count - 1 - k if reverse else k, carry)
        return carry

    return lax.fori_loop(0, count // unroll, block, init)


def kernel(
    ny_parts, half,
    u_in, pc_in, lc_in, src_in, table, index,
    out,
    u_x, pc_x, lc_x, src_x, to_left, to_right, from_left, from_right,
    p_s, pr_s, b_s, f_s, iq_s, beta_s, beta_r, face_s, face_r,
    in_sem, xs_sem, xr_sem, ys_sem, yr_sem, bs_sem, br_sem, fs_sem, fr_sem,
):
    n, rows, lanes = u_in.shape
    width = half
    per = lanes // width
    groups = n // per
    gz, gx, gy = lax.axis_index("gz"), lax.axis_index("gx"), lax.axis_index("gy")
    has_left, has_right = gy > 0, gy < ny_parts - 1
    own_r, own_c = pl.ds(0, rows), pl.ds(0, lanes)
    other_r, halo_c = pl.ds(rows, rows), pl.ds(lanes, lanes)
    all_r = pl.ds(0, 2 * rows)
    ins = (u_in, pc_in, lc_in, src_in)
    exts = (u_x, pc_x, lc_x, src_x)

    loads = [
        pltpu.make_async_copy(i, e.at[:, own_r, own_c], in_sem.at[a])
        for a, (i, e) in enumerate(zip(ins, exts))
    ]
    for c in loads:
        c.start()

    barrier = pltpu.get_barrier_semaphore()

    def greet(device):
        pl.semaphore_signal(
            barrier, inc=1, device_id=device, device_id_type=pl.DeviceIdType.MESH
        )

    x_peer = (gz, 1 - gx, gy)
    z_peer = (1 - gz, gx, gy)
    left = ((gz, gx, gy - 1), (gz, 1 - gx, gy - 1))
    right = ((gz, gx, gy + 1), (gz, 1 - gx, gy + 1))
    greet(x_peer)
    greet(z_peer)

    @pl.when(has_left)
    def _():
        greet(left[0])
        greet(left[1])

    @pl.when(has_right)
    def _():
        greet(right[0])
        greet(right[1])

    for c in loads:
        c.wait()

    lane = lax.broadcasted_iota(jnp.int32, (rows, lanes), 1)

    def slot(j):
        return (lane >= j * width) & (lane < j * width + width)

    def pack(j, carry):
        at_right = slot(j)
        at_left = slot((j + 1) % per)
        done = []
        for i, (e, g) in enumerate((e, g) for e in exts for g in range(groups)):
            t = pltpu.roll(e[g * per + j, own_r, own_c], ((j + 1) % per) * width, 1)
            r, l = carry[i]
            done.append((jnp.where(at_right, t, r), jnp.where(at_left, t, l)))
        return tuple(done)

    zero = jnp.zeros((rows, lanes), jnp.float32)
    packed = loop(per, pack, tuple((zero, zero) for _ in range(4 * groups)), 2)
    for i, (r, l) in enumerate(packed):
        to_right[i] = r
        to_left[i] = l

    lefts_there = (gy + ny_parts - 1) // ny_parts
    rights_there = (2 * ny_parts - 2 - gy) // ny_parts
    pl.semaphore_wait(barrier, 2 + 2 * lefts_there + 2 * rights_there)

    def remote(src, dst, send, recv, device):
        return pltpu.make_async_remote_copy(
            src_ref=src, dst_ref=dst, send_sem=send, recv_sem=recv,
            device_id=device, device_id_type=pl.DeviceIdType.MESH,
        )

    lefts = [
        remote(to_left, from_right.at[t], ys_sem.at[t], yr_sem.at[t], left[t]) for t in range(2)
    ]
    rights = [
        remote(to_right, from_left.at[t], ys_sem.at[2 + t], yr_sem.at[2 + t], right[t])
        for t in range(2)
    ]

    @pl.when(has_left)
    def _():
        for c in lefts:
            c.start()

    @pl.when(has_right)
    def _():
        for c in rights:
            c.start()

    xs = [
        remote(
            e.at[:, own_r, own_c], e.at[:, other_r, own_c], xs_sem.at[a], xr_sem.at[a], x_peer
        )
        for a, e in enumerate(exts)
    ]
    for a in (2, 0, 1, 3):
        xs[a].start()

    def layer(k):
        return k + gz * (n - 1 - 2 * k)

    def shift(h):
        return table[index[h]]

    def inverse(h, shape):
        return 1.0 / jnp.full(shape, shift(h), jnp.float32)

    def factor(r_at, c_at, hs, unroll):
        shape = (r_at.size, lanes)
        inv = inverse_all(hs, shape)
        one = jnp.ones(shape, jnp.float32)

        def body(k, carry):
            z = layer(k)
            rl = 1.0 / lc_x[z, r_at, c_at]
            done = []
            for (p, d), h, i in zip(carry, hs, inv):
                d = d + (rl * i) * p
                q = p + d
                p_s[h, z, r_at, c_at] = p
                pr_s[h, z, r_at, c_at] = p * rl
                b_s[h, z, r_at, c_at] = 1.0 / (p * q)
                done.append((q, d))
            return tuple(done)

        final = loop(n, body, tuple((one, one) for _ in hs), unroll)
        for (q, d), h in zip(final, hs):
            iq = 1.0 / q
            iq_s[h, r_at, c_at] = iq
            beta_s[h, r_at, c_at] = d * iq

    def inverse_all(hs, shape):
        return [inverse(h, shape) for h in hs]

    steps = list(range(half))
    factor(own_r, own_c, steps, 2)
    for a in (2, 0, 1, 3):
        xs[a].wait()
    factor(other_r, own_c, steps[:-1], 2)

    def send_beta(h, c_at, i):
        return remote(
            beta_s.at[h, :, c_at], beta_r.at[h, :, c_at], bs_sem.at[i], br_sem.at[i], z_peer
        )

    last = half - 1
    betas = [[send_beta(h, own_c, h)] for h in steps[:-1]]
    betas.append(
        [remote(
            beta_s.at[last, own_r, own_c], beta_r.at[last, own_r, own_c],
            bs_sem.at[last], br_sem.at[last], z_peer,
        )]
    )
    for b in betas:
        b[0].start()

    @pl.when(has_left)
    def _():
        for c in lefts:
            c.wait_send()
        for c in rights:
            c.wait_recv()

    @pl.when(has_right)
    def _():
        for c in rights:
            c.wait_send()
        for c in lefts:
            c.wait_recv()

    inside = ((lane < width) & has_right) | ((lane >= lanes - width) & has_left)

    def unpack(j, carry):
        at_left = slot((j + 1) % per)
        back = ((per - 1 - j) % per) * width
        for t in range(2):
            r_at = pl.ds(t * rows, rows)
            for a, e in enumerate(exts):
                for g in range(groups):
                    i = a * groups + g
                    both = jnp.where(at_left, from_right[t, i], from_left[t, i])
                    z = g * per + j
                    rest = lc_x[z, r_at, own_c] if a == 2 else jnp.zeros((rows, lanes), jnp.float32)
                    e[z, r_at, halo_c] = jnp.where(inside, pltpu.roll(both, back, 1), rest)
        return carry

    loop(per, unpack, 0, 1)

    def factor_halo(h):
        factor(all_r, halo_c, [h], 2)
        c = send_beta(h, halo_c, half + h)
        c.start()
        betas[h].append(c)

    factor_halo(0)

    wide = (2 * rows, 2 * lanes)
    row = lax.broadcasted_iota(jnp.int32, wide, 0)
    top = row == gx * rows
    bottom = row == (2 * rows - 1 + gx * rows) % (2 * rows)

    for h in steps:
        final = h == last
        r_at, c_at = (own_r, own_c) if final else (all_r, pl.ds(0, 2 * lanes))
        cut = (lambda a: a[:rows, :lanes]) if final else (lambda a: a)
        shape = (rows, lanes) if final else wide
        inv = inverse(h, shape)

        def ahead(k, total, h=h, inv=inv, cut=cut, r_at=r_at, c_at=c_at):
            z = layer(k)
            u = u_x[z]
            beside = (
                jnp.where(top, 0.0, pltpu.roll(u, 1, 0))
                + jnp.where(bottom, 0.0, pltpu.roll(u, 2 * rows - 1, 0))
                + pltpu.roll(u, 1, 1)
                + pltpu.roll(u, 2 * lanes - 1, 1)
            )
            u = cut(u)
            e = u * inv + (pc_x[z, r_at, c_at] * (cut(beside) - 4.0 * u) + src_x[z, r_at, c_at])
            total = total + pr_s[h, z, r_at, c_at] * e
            f_s[z, r_at, c_at] = total
            return total

        total = loop(n, ahead, jnp.zeros(shape, jnp.float32), 4)
        iq = iq_s[h, r_at, c_at]
        face = total * iq
        face_s[h, r_at, c_at] = face
        send = remote(
            face_s.at[h, r_at, c_at], face_r.at[h, r_at, c_at], fs_sem.at[h], fr_sem.at[h], z_peer
        )
        send.start()
        if h + 1 < last:
            factor_halo(h + 1)
        for b in betas[h]:
            b.wait()
        mine, theirs = beta_s[h, r_at, c_at], beta_r[h, r_at, c_at]
        gain = iq / (mine + theirs - mine * theirs)
        partial = (1.0 - theirs) * face
        send.wait()
        v = (face_r[h, r_at, c_at] + partial) * gain

        def behind(k, v, h=h, final=final, r_at=r_at, c_at=c_at):
            z = layer(k)
            v = v + f_s[z, r_at, c_at] * b_s[h, z, r_at, c_at]
            w = p_s[h, z, r_at, c_at] * v
            if final:
                out[z] = w
            else:
                u_x[z] = w
            return v

        loop(n, behind, v, 4, reverse=True)


def solution(mesh):
    ny_parts = mesh.shape["gy"]
    assert mesh.shape["gz"] == 2 and mesh.shape["gx"] == 2

    def on_device(u, pc, lc, src, table, index):
        half = index.shape[0]
        n, rows, lanes = u.shape
        f32 = jnp.float32
        ext = pltpu.VMEM((n, 2 * rows, 2 * lanes), f32)
        coef = pltpu.VMEM((half, n, 2 * rows, 2 * lanes), f32)
        face = pltpu.VMEM((half, 2 * rows, 2 * lanes), f32)
        count = 4 * (n * half // lanes)
        pack = pltpu.VMEM((count, rows, lanes), f32)
        packs = pltpu.VMEM((2, count, rows, lanes), f32)
        dma = pltpu.SemaphoreType.DMA
        return pl.pallas_call(
            functools.partial(kernel, ny_parts, half),
            out_shape=jax.ShapeDtypeStruct(u.shape, f32),
            in_specs=[pl.BlockSpec(memory_space=pl.ANY)] * 4
            + [pl.BlockSpec(memory_space=pltpu.SMEM)] * 2,
            out_specs=pl.BlockSpec(memory_space=pltpu.VMEM),
            scratch_shapes=[ext] * 4 + [pack] * 2 + [packs] * 2
            + [coef] * 3 + [ext] + [face] * 5
            + [dma((4,)), dma((4,)), dma((4,)), dma((4,)), dma((4,)),
               dma((2 * half,)), dma((2 * half,)), dma((half,)), dma((half,))],
            compiler_params=pltpu.CompilerParams(collective_id=0, has_side_effects=True),
        )(u, pc, lc, src, table, index)

    spec = P("gz", "gx", "gy")
    return jax.shard_map(
        on_device, mesh=mesh, in_specs=(spec,) * 4 + (P(), P()), out_specs=spec, check_vma=False
    )
```

```python
import functools

import jax
import jax.numpy as jnp
from jax import lax
from jax.experimental import pallas as pl
from jax.experimental.pallas import tpu as pltpu
from jax.sharding import PartitionSpec as P


EXPLICIT = 16
SUMS = 8
PACK = 4
UNPACK = 4
FACTOR = 2


def loop(count, body, init, unroll, reverse=False):
    while count % unroll:
        unroll -= 1

    def block(i, carry):
        for j in range(unroll):
            k = i * unroll + j
            carry = body(count - 1 - k if reverse else k, carry)
        return carry

    return lax.fori_loop(0, count // unroll, block, init)


def kernel(
    ny_parts, half,
    u_in, pc_in, lc_in, src_in, table, index,
    out,
    u_x, pc_x, lc_x, src_x, to_left, to_right, from_left, from_right,
    p_s, pr_s, b_s, f_s, iq_s, beta_s, beta_r, face_s, face_r,
    in_sem, xs_sem, xr_sem, ys_sem, yr_sem, bs_sem, br_sem, fs_sem, fr_sem,
):
    n, rows, lanes = u_in.shape
    width = half
    per = lanes // width
    groups = n // per
    gz, gx, gy = lax.axis_index("gz"), lax.axis_index("gx"), lax.axis_index("gy")
    has_left, has_right = gy > 0, gy < ny_parts - 1
    own_r, own_c = pl.ds(0, rows), pl.ds(0, lanes)
    other_r, halo_c = pl.ds(rows, rows), pl.ds(lanes, lanes)
    all_r = pl.ds(0, 2 * rows)
    ins = (u_in, pc_in, lc_in, src_in)
    exts = (u_x, pc_x, lc_x, src_x)

    loads = [
        pltpu.make_async_copy(i, e.at[:, own_r, own_c], in_sem.at[a])
        for a, (i, e) in enumerate(zip(ins, exts))
    ]
    for c in loads:
        c.start()

    barrier = pltpu.get_barrier_semaphore()

    def greet(device):
        pl.semaphore_signal(
            barrier, inc=1, device_id=device, device_id_type=pl.DeviceIdType.MESH
        )

    x_peer = (gz, 1 - gx, gy)
    z_peer = (1 - gz, gx, gy)
    left = ((gz, gx, gy - 1), (gz, 1 - gx, gy - 1))
    right = ((gz, gx, gy + 1), (gz, 1 - gx, gy + 1))
    greet(x_peer)
    greet(z_peer)

    @pl.when(has_left)
    def _():
        greet(left[0])
        greet(left[1])

    @pl.when(has_right)
    def _():
        greet(right[0])
        greet(right[1])

    for c in loads:
        c.wait()

    lane = lax.broadcasted_iota(jnp.int32, (rows, lanes), 1)

    def slot(j):
        return (lane >= j * width) & (lane < j * width + width)

    def pack(j, carry):
        at_right = slot(j)
        at_left = slot((j + 1) % per)
        done = []
        for i, (e, g) in enumerate((e, g) for e in exts for g in range(groups)):
            t = pltpu.roll(e[g * per + j, own_r, own_c], ((j + 1) % per) * width, 1)
            r, l = carry[i]
            done.append((jnp.where(at_right, t, r), jnp.where(at_left, t, l)))
        return tuple(done)

    zero = jnp.zeros((rows, lanes), jnp.float32)
    packed = loop(per, pack, tuple((zero, zero) for _ in range(4 * groups)), PACK)
    for i, (r, l) in enumerate(packed):
        to_right[i] = r
        to_left[i] = l

    lefts_there = (gy + ny_parts - 1) // ny_parts
    rights_there = (2 * ny_parts - 2 - gy) // ny_parts
    pl.semaphore_wait(barrier, 2 + 2 * lefts_there + 2 * rights_there)

    def remote(src, dst, send, recv, device):
        return pltpu.make_async_remote_copy(
            src_ref=src, dst_ref=dst, send_sem=send, recv_sem=recv,
            device_id=device, device_id_type=pl.DeviceIdType.MESH,
        )

    lefts = [
        remote(to_left, from_right.at[t], ys_sem.at[t], yr_sem.at[t], left[t]) for t in range(2)
    ]
    rights = [
        remote(to_right, from_left.at[t], ys_sem.at[2 + t], yr_sem.at[2 + t], right[t])
        for t in range(2)
    ]

    @pl.when(has_left)
    def _():
        for c in lefts:
            c.start()

    @pl.when(has_right)
    def _():
        for c in rights:
            c.start()

    xs = [
        remote(
            e.at[:, own_r, own_c], e.at[:, other_r, own_c], xs_sem.at[a], xr_sem.at[a], x_peer
        )
        for a, e in enumerate(exts)
    ]
    for a in (2, 0, 1, 3):
        xs[a].start()

    def layer(k):
        return k + gz * (n - 1 - 2 * k)

    def shift(h):
        return table[index[h]]

    def inverse(h, shape):
        return 1.0 / jnp.full(shape, shift(h), jnp.float32)

    def factor(r_at, c_at, hs):
        shape = (r_at.size, lanes)
        inv = inverse_all(hs, shape)
        one = jnp.ones(shape, jnp.float32)

        def body(k, carry):
            z = layer(k)
            rl = 1.0 / lc_x[z, r_at, c_at]
            done = []
            for (p, d), h, i in zip(carry, hs, inv):
                d = d + (rl * i) * p
                q = p + d
                p_s[h, z, r_at, c_at] = p
                pr_s[h, z, r_at, c_at] = p * rl
                b_s[h, z, r_at, c_at] = 1.0 / (p * q)
                done.append((q, d))
            return tuple(done)

        final = loop(n, body, tuple((one, one) for _ in hs), FACTOR)
        for (q, d), h in zip(final, hs):
            iq = 1.0 / q
            iq_s[h, r_at, c_at] = iq
            beta_s[h, r_at, c_at] = d * iq

    def inverse_all(hs, shape):
        return [inverse(h, shape) for h in hs]

    steps = list(range(half))
    factor(own_r, own_c, steps)
    for a in (2, 0, 1, 3):
        xs[a].wait()
    factor(other_r, own_c, steps[:-1])

    def send_beta(h, c_at, i):
        return remote(
            beta_s.at[h, :, c_at], beta_r.at[h, :, c_at], bs_sem.at[i], br_sem.at[i], z_peer
        )

    last = half - 1
    betas = [[send_beta(h, own_c, h)] for h in steps[:-1]]
    betas.append(
        [remote(
            beta_s.at[last, own_r, own_c], beta_r.at[last, own_r, own_c],
            bs_sem.at[last], br_sem.at[last], z_peer,
        )]
    )
    for b in betas:
        b[0].start()

    @pl.when(has_left)
    def _():
        for c in lefts:
            c.wait_send()
        for c in rights:
            c.wait_recv()

    @pl.when(has_right)
    def _():
        for c in rights:
            c.wait_send()
        for c in lefts:
            c.wait_recv()

    inside = ((lane < width) & has_right) | ((lane >= lanes - width) & has_left)

    def unpack(j, carry):
        at_left = slot((j + 1) % per)
        back = ((per - 1 - j) % per) * width
        for t in range(2):
            r_at = pl.ds(t * rows, rows)
            for a, e in enumerate(exts):
                for g in range(groups):
                    i = a * groups + g
                    both = jnp.where(at_left, from_right[t, i], from_left[t, i])
                    z = g * per + j
                    rest = lc_x[z, r_at, own_c] if a == 2 else jnp.zeros((rows, lanes), jnp.float32)
                    e[z, r_at, halo_c] = jnp.where(inside, pltpu.roll(both, back, 1), rest)
        return carry

    loop(per, unpack, 0, UNPACK)

    def factor_halo(h):
        factor(all_r, halo_c, [h])
        c = send_beta(h, halo_c, half + h)
        c.start()
        betas[h].append(c)

    factor_halo(0)

    wide = (2 * rows, 2 * lanes)
    row = lax.broadcasted_iota(jnp.int32, wide, 0)
    top = row == gx * rows
    bottom = row == (2 * rows - 1 + gx * rows) % (2 * rows)

    def edges(u):
        return (
            jnp.where(top, 0.0, pltpu.roll(u, 1, 0))
            + jnp.where(bottom, 0.0, pltpu.roll(u, 2 * rows - 1, 0))
            + pltpu.roll(u, 1, 1)
            + pltpu.roll(u, 2 * lanes - 1, 1)
        )

    def explicit(h, field):
        r_at, c_at, shape, cut = part(h)
        inv = inverse(h, shape)

        def body(k, total):
            z = layer(k)
            u = field(z)
            beside = cut(edges(u))
            u = cut(u)
            e = u * inv + (pc_x[z, r_at, c_at] * (beside - 4.0 * u) + src_x[z, r_at, c_at])
            g = pr_s[h, z, r_at, c_at] * e
            f_s[z, r_at, c_at] = g
            return total + g

        return loop(n, body, jnp.zeros(shape, jnp.float32), EXPLICIT)

    def part(h):
        if h == last:
            return own_r, own_c, (rows, lanes), lambda a: a[:rows, :lanes]
        return all_r, pl.ds(0, 2 * lanes), wide, lambda a: a

    total = explicit(0, lambda z: u_x[z])
    for h in steps:
        r_at, c_at, shape, _ = part(h)
        iq = iq_s[h, r_at, c_at]
        face = total * iq
        face_s[h, r_at, c_at] = face
        send = remote(
            face_s.at[h, r_at, c_at], face_r.at[h, r_at, c_at], fs_sem.at[h], fr_sem.at[h], z_peer
        )
        send.start()
        zero_part = jnp.zeros(shape, jnp.float32)

        def ahead(k, total, h=h, r_at=r_at, c_at=c_at):
            z = layer(k)
            total = total + f_s[z, r_at, c_at]
            f_s[z, r_at, c_at] = total * b_s[h, z, r_at, c_at]
            return total

        def behind(k, total, h=h, r_at=r_at, c_at=c_at):
            z = layer(k)
            total = total + f_s[z, r_at, c_at]
            f_s[z, r_at, c_at] = p_s[h, z, r_at, c_at] * total
            return total

        loop(n, ahead, zero_part, SUMS)
        loop(n, behind, zero_part, SUMS, reverse=True)
        if h + 1 < last:
            factor_halo(h + 1)
        for b in betas[h]:
            b.wait()
        mine, theirs = beta_s[h, r_at, c_at], beta_r[h, r_at, c_at]
        gain = iq / (mine + theirs - mine * theirs)
        partial = (1.0 - theirs) * face
        send.wait()
        v = (face_r[h, r_at, c_at] + partial) * gain

        def solved(z, h=h, v=v, r_at=r_at, c_at=c_at):
            return p_s[h, z, r_at, c_at] * v + f_s[z, r_at, c_at]

        if h < last:
            total = explicit(h + 1, solved)
        else:

            def write(z, carry):
                out[z] = solved(z)
                return carry

            loop(n, write, 0, SUMS)


def solution(mesh):
    ny_parts = mesh.shape["gy"]
    assert mesh.shape["gz"] == 2 and mesh.shape["gx"] == 2

    def on_device(u, pc, lc, src, table, index):
        half = index.shape[0]
        n, rows, lanes = u.shape
        f32 = jnp.float32
        ext = pltpu.VMEM((n, 2 * rows, 2 * lanes), f32)
        coef = pltpu.VMEM((half, n, 2 * rows, 2 * lanes), f32)
        face = pltpu.VMEM((half, 2 * rows, 2 * lanes), f32)
        count = 4 * (n * half // lanes)
        pack = pltpu.VMEM((count, rows, lanes), f32)
        packs = pltpu.VMEM((2, count, rows, lanes), f32)
        dma = pltpu.SemaphoreType.DMA
        return pl.pallas_call(
            functools.partial(kernel, ny_parts, half),
            out_shape=jax.ShapeDtypeStruct(u.shape, f32),
            in_specs=[pl.BlockSpec(memory_space=pl.ANY)] * 4
            + [pl.BlockSpec(memory_space=pltpu.SMEM)] * 2,
            out_specs=pl.BlockSpec(memory_space=pltpu.VMEM),
            scratch_shapes=[ext] * 4 + [pack] * 2 + [packs] * 2
            + [coef] * 3 + [ext] + [face] * 5
            + [dma((4,)), dma((4,)), dma((4,)), dma((4,)), dma((4,)),
               dma((2 * half,)), dma((2 * half,)), dma((half,)), dma((half,))],
            compiler_params=pltpu.CompilerParams(collective_id=0, has_side_effects=True),
        )(u, pc, lc, src, table, index)

    spec = P("gz", "gx", "gy")
    return jax.shard_map(
        on_device, mesh=mesh, in_specs=(spec,) * 4 + (P(), P()), out_specs=spec, check_vma=False
    )
```

```python
import functools

import jax
import jax.numpy as jnp
from jax import lax
from jax.experimental import pallas as pl
from jax.experimental.pallas import tpu as pltpu
from jax.sharding import PartitionSpec as P


EXPLICIT = 16
SUMS = 8
PACK = 4
UNPACK = 4
FACTOR = 2


def loop(count, body, init, unroll, reverse=False):
    while count % unroll:
        unroll -= 1

    def block(i, carry):
        for j in range(unroll):
            k = i * unroll + j
            carry = body(count - 1 - k if reverse else k, carry)
        return carry

    return lax.fori_loop(0, count // unroll, block, init)


def kernel(
    ny_parts, half,
    u_in, pc_in, lc_in, src_in, table, index,
    out,
    u_x, pc_x, lc_x, src_x, to_left, to_right, from_left, from_right,
    p_s, pr_s, b_s, g_s, f_s, w_s, iq_s, beta_s, beta_r, face_s, face_r,
    in_sem, xs_sem, xr_sem, ys_sem, yr_sem, bs_sem, br_sem, fs_sem, fr_sem,
):
    n, rows, lanes = u_in.shape
    width = half
    per = lanes // width
    groups = n // per
    gz, gx, gy = lax.axis_index("gz"), lax.axis_index("gx"), lax.axis_index("gy")
    has_left, has_right = gy > 0, gy < ny_parts - 1
    own_r, own_c = pl.ds(0, rows), pl.ds(0, lanes)
    other_r, halo_c = pl.ds(rows, rows), pl.ds(lanes, lanes)
    all_r = pl.ds(0, 2 * rows)
    ins = (u_in, pc_in, lc_in, src_in)
    exts = (u_x, pc_x, lc_x, src_x)

    loads = [
        pltpu.make_async_copy(i, e.at[:, own_r, own_c], in_sem.at[a])
        for a, (i, e) in enumerate(zip(ins, exts))
    ]
    for c in loads:
        c.start()

    barrier = pltpu.get_barrier_semaphore()

    def greet(device):
        pl.semaphore_signal(
            barrier, inc=1, device_id=device, device_id_type=pl.DeviceIdType.MESH
        )

    x_peer = (gz, 1 - gx, gy)
    z_peer = (1 - gz, gx, gy)
    left = ((gz, gx, gy - 1), (gz, 1 - gx, gy - 1))
    right = ((gz, gx, gy + 1), (gz, 1 - gx, gy + 1))
    greet(x_peer)
    greet(z_peer)

    @pl.when(has_left)
    def _():
        greet(left[0])
        greet(left[1])

    @pl.when(has_right)
    def _():
        greet(right[0])
        greet(right[1])

    for c in loads:
        c.wait()

    lane = lax.broadcasted_iota(jnp.int32, (rows, lanes), 1)

    def slot(j):
        return (lane >= j * width) & (lane < j * width + width)

    def pack(j, carry):
        at_right = slot(j)
        at_left = slot(lax.rem(j + 1, per))
        done = []
        for i, (e, g) in enumerate((e, g) for e in exts for g in range(groups)):
            t = pltpu.roll(e[g * per + j, own_r, own_c], (lax.rem(j + 1, per)) * width, 1)
            r, l = carry[i]
            done.append((jnp.where(at_right, t, r), jnp.where(at_left, t, l)))
        return tuple(done)

    zero = jnp.zeros((rows, lanes), jnp.float32)
    packed = loop(per, pack, tuple((zero, zero) for _ in range(4 * groups)), PACK)
    for i, (r, l) in enumerate(packed):
        to_right[i] = r
        to_left[i] = l

    lefts_there = (gy + ny_parts - 1) // ny_parts
    rights_there = (2 * ny_parts - 2 - gy) // ny_parts
    pl.semaphore_wait(barrier, 2 + 2 * lefts_there + 2 * rights_there)

    def remote(src, dst, send, recv, device):
        return pltpu.make_async_remote_copy(
            src_ref=src, dst_ref=dst, send_sem=send, recv_sem=recv,
            device_id=device, device_id_type=pl.DeviceIdType.MESH,
        )

    lefts = [
        remote(to_left, from_right.at[t], ys_sem.at[t], yr_sem.at[t], left[t]) for t in range(2)
    ]
    rights = [
        remote(to_right, from_left.at[t], ys_sem.at[2 + t], yr_sem.at[2 + t], right[t])
        for t in range(2)
    ]

    @pl.when(has_left)
    def _():
        for c in lefts:
            c.start()

    @pl.when(has_right)
    def _():
        for c in rights:
            c.start()

    xs = [
        remote(
            e.at[:, own_r, own_c], e.at[:, other_r, own_c], xs_sem.at[a], xr_sem.at[a], x_peer
        )
        for a, e in enumerate(exts)
    ]
    for a in (2, 0, 1, 3):
        xs[a].start()

    def layer(k):
        return k + gz * (n - 1 - 2 * k)

    def shift(h):
        return table[index[h]]

    def inverse(h, shape):
        return 1.0 / jnp.full(shape, shift(h), jnp.float32)

    def factor(r_at, c_at, hs):
        shape = (r_at.size, lanes)
        inv = inverse_all(hs, shape)
        one = jnp.ones(shape, jnp.float32)

        def body(k, carry):
            z = layer(k)
            rl = 1.0 / lc_x[z, r_at, c_at]
            done = []
            for (p, d), h, i in zip(carry, hs, inv):
                d = d + (rl * i) * p
                q = p + d
                p_s[h, z, r_at, c_at] = p
                pr_s[h, z, r_at, c_at] = p * rl
                b_s[h, z, r_at, c_at] = 1.0 / (p * q)
                done.append((q, d))
            return tuple(done)

        final = loop(n, body, tuple((one, one) for _ in hs), FACTOR)
        for (q, d), h in zip(final, hs):
            iq = 1.0 / q
            iq_s[h, r_at, c_at] = iq
            beta_s[h, r_at, c_at] = d * iq

    def inverse_all(hs, shape):
        return [inverse(h, shape) for h in hs]

    steps = list(range(half))
    factor(own_r, own_c, steps)
    for a in (2, 0, 1, 3):
        xs[a].wait()
    factor(other_r, own_c, steps[:-1])

    def send_beta(h, c_at, i):
        return remote(
            beta_s.at[h, :, c_at], beta_r.at[h, :, c_at], bs_sem.at[i], br_sem.at[i], z_peer
        )

    last = half - 1
    betas = [[send_beta(h, own_c, h)] for h in steps[:-1]]
    betas.append(
        [remote(
            beta_s.at[last, own_r, own_c], beta_r.at[last, own_r, own_c],
            bs_sem.at[last], br_sem.at[last], z_peer,
        )]
    )
    for b in betas:
        b[0].start()

    @pl.when(has_left)
    def _():
        for c in lefts:
            c.wait_send()
        for c in rights:
            c.wait_recv()

    @pl.when(has_right)
    def _():
        for c in rights:
            c.wait_send()
        for c in lefts:
            c.wait_recv()

    inside = ((lane < width) & has_right) | ((lane >= lanes - width) & has_left)

    filler = lc_x[0, own_r, own_c]

    def unpack(j, carry):
        at_left = slot(lax.rem(j + 1, per))
        back = (per - 1 - j) * width
        for t in range(2):
            r_at = pl.ds(t * rows, rows)
            for a, e in enumerate(exts):
                for g in range(groups):
                    i = a * groups + g
                    both = jnp.where(at_left, from_right[t, i], from_left[t, i])
                    z = g * per + j
                    rest = filler if a == 2 else zero
                    e[z, r_at, halo_c] = jnp.where(inside, pltpu.roll(both, back, 1), rest)
        return carry

    loop(per, unpack, 0, UNPACK)

    def factor_halo(h):
        factor(all_r, halo_c, [h])
        c = send_beta(h, halo_c, half + h)
        c.start()
        betas[h].append(c)

    factor_halo(0)

    wide = (2 * rows, 2 * lanes)
    row = lax.broadcasted_iota(jnp.int32, wide, 0)
    top = row == gx * rows
    bottom = row == (2 * rows - 1 + gx * rows) % (2 * rows)

    def edges(u):
        return (
            jnp.where(top, 0.0, pltpu.roll(u, 1, 0))
            + jnp.where(bottom, 0.0, pltpu.roll(u, 2 * rows - 1, 0))
            + pltpu.roll(u, 1, 1)
            + pltpu.roll(u, 2 * lanes - 1, 1)
        )

    def explicit(h, field):
        r_at, c_at, shape, cut = part(h)
        inv = inverse(h, shape)

        def body(k, total):
            z = layer(k)
            u = field(z)
            beside = cut(edges(u))
            u = cut(u)
            e = u * inv + (pc_x[z, r_at, c_at] * (beside - 4.0 * u) + src_x[z, r_at, c_at])
            g = pr_s[h, z, r_at, c_at] * e
            g_s[z, r_at, c_at] = g
            return total + g

        return loop(n, body, jnp.zeros(shape, jnp.float32), EXPLICIT)

    def part(h):
        if h == last:
            return own_r, own_c, (rows, lanes), lambda a: a[:rows, :lanes]
        return all_r, pl.ds(0, 2 * lanes), wide, lambda a: a

    total = explicit(0, lambda z: u_x[z])
    for h in steps:
        r_at, c_at, shape, _ = part(h)
        iq = iq_s[h, r_at, c_at]
        face = total * iq
        face_s[h, r_at, c_at] = face
        send = remote(
            face_s.at[h, r_at, c_at], face_r.at[h, r_at, c_at], fs_sem.at[h], fr_sem.at[h], z_peer
        )
        send.start()
        zero_part = jnp.zeros(shape, jnp.float32)

        def ahead(k, total, h=h, r_at=r_at, c_at=c_at):
            z = layer(k)
            total = total + g_s[z, r_at, c_at]
            f_s[z, r_at, c_at] = total * b_s[h, z, r_at, c_at]
            return total

        def behind(k, total, h=h, r_at=r_at, c_at=c_at):
            z = layer(k)
            total = total + f_s[z, r_at, c_at]
            w_s[z, r_at, c_at] = p_s[h, z, r_at, c_at] * total
            return total

        loop(n, ahead, zero_part, SUMS)
        loop(n, behind, zero_part, SUMS, reverse=True)
        if h + 1 < last:
            factor_halo(h + 1)
        for b in betas[h]:
            b.wait()
        mine, theirs = beta_s[h, r_at, c_at], beta_r[h, r_at, c_at]
        gain = iq / (mine + theirs - mine * theirs)
        partial = (1.0 - theirs) * face
        send.wait()
        v = (face_r[h, r_at, c_at] + partial) * gain

        def solved(z, h=h, v=v, r_at=r_at, c_at=c_at):
            return p_s[h, z, r_at, c_at] * v + w_s[z, r_at, c_at]

        if h < last:
            total = explicit(h + 1, solved)
        else:

            def write(z, carry):
                out[z] = solved(z)
                return carry

            loop(n, write, 0, SUMS)


def solution(mesh):
    ny_parts = mesh.shape["gy"]
    assert mesh.shape["gz"] == 2 and mesh.shape["gx"] == 2

    def on_device(u, pc, lc, src, table, index):
        half = index.shape[0]
        n, rows, lanes = u.shape
        f32 = jnp.float32
        ext = pltpu.VMEM((n, 2 * rows, 2 * lanes), f32)
        coef = pltpu.VMEM((half, n, 2 * rows, 2 * lanes), f32)
        face = pltpu.VMEM((half, 2 * rows, 2 * lanes), f32)
        count = 4 * (n * half // lanes)
        pack = pltpu.VMEM((count, rows, lanes), f32)
        packs = pltpu.VMEM((2, count, rows, lanes), f32)
        dma = pltpu.SemaphoreType.DMA
        return pl.pallas_call(
            functools.partial(kernel, ny_parts, half),
            out_shape=jax.ShapeDtypeStruct(u.shape, f32),
            in_specs=[pl.BlockSpec(memory_space=pl.ANY)] * 4
            + [pl.BlockSpec(memory_space=pltpu.SMEM)] * 2,
            out_specs=pl.BlockSpec(memory_space=pltpu.VMEM),
            scratch_shapes=[ext] * 4 + [pack] * 2 + [packs] * 2
            + [coef] * 3 + [ext] * 3 + [face] * 5
            + [dma((4,)), dma((4,)), dma((4,)), dma((4,)), dma((4,)),
               dma((2 * half,)), dma((2 * half,)), dma((half,)), dma((half,))],
            compiler_params=pltpu.CompilerParams(collective_id=0, has_side_effects=True),
        )(u, pc, lc, src, table, index)

    spec = P("gz", "gx", "gy")
    return jax.shard_map(
        on_device, mesh=mesh, in_specs=(spec,) * 4 + (P(), P()), out_specs=spec, check_vma=False
    )
```

```python
import functools

import jax
import jax.numpy as jnp
from jax import lax
from jax.experimental import pallas as pl
from jax.experimental.pallas import tpu as pltpu
from jax.sharding import PartitionSpec as P


EXPLICIT = 32
SUMS = 8
PACK = 16
UNPACK = 16
FACTOR = 8


def loop(count, body, init, unroll, reverse=False):
    while count % unroll:
        unroll -= 1

    def block(i, carry):
        for j in range(unroll):
            k = i * unroll + j
            carry = body(count - 1 - k if reverse else k, carry)
        return carry

    return lax.fori_loop(0, count // unroll, block, init)


def kernel(
    ny_parts, half,
    u_in, pc_in, lc_in, src_in, table, index,
    out,
    u_x, pc_x, lc_x, src_x, to_left, to_right, from_left, from_right,
    p_s, own_s, near_s, src_s, b_s, g_s, f_s, w_s, iq_s, beta_s, beta_r, face_s, face_r,
    in_sem, xs_sem, xr_sem, ys_sem, yr_sem, bs_sem, br_sem, fs_sem, fr_sem,
):
    n, rows, lanes = u_in.shape
    width = half
    per = lanes // width
    groups = n // per
    gz, gx, gy = lax.axis_index("gz"), lax.axis_index("gx"), lax.axis_index("gy")
    has_left, has_right = gy > 0, gy < ny_parts - 1
    own_r, own_c = pl.ds(0, rows), pl.ds(0, lanes)
    other_r, halo_c = pl.ds(rows, rows), pl.ds(lanes, lanes)
    all_r = pl.ds(0, 2 * rows)
    ins = (u_in, pc_in, lc_in, src_in)
    exts = (u_x, pc_x, lc_x, src_x)

    loads = [
        pltpu.make_async_copy(i, e.at[:, own_r, own_c], in_sem.at[a])
        for a, (i, e) in enumerate(zip(ins, exts))
    ]
    for c in loads:
        c.start()

    barrier = pltpu.get_barrier_semaphore()

    def greet(device):
        pl.semaphore_signal(
            barrier, inc=1, device_id=device, device_id_type=pl.DeviceIdType.MESH
        )

    x_peer = (gz, 1 - gx, gy)
    z_peer = (1 - gz, gx, gy)
    left = ((gz, gx, gy - 1), (gz, 1 - gx, gy - 1))
    right = ((gz, gx, gy + 1), (gz, 1 - gx, gy + 1))
    greet(x_peer)
    greet(z_peer)

    @pl.when(has_left)
    def _():
        greet(left[0])
        greet(left[1])

    @pl.when(has_right)
    def _():
        greet(right[0])
        greet(right[1])

    for c in loads:
        c.wait()

    lane = lax.broadcasted_iota(jnp.int32, (rows, lanes), 1)

    def slot(j):
        return (lane >= j * width) & (lane < j * width + width)

    def pack(j, carry):
        at_right = slot(j)
        at_left = slot(lax.rem(j + 1, per))
        done = []
        for i, (e, g) in enumerate((e, g) for e in exts for g in range(groups)):
            t = pltpu.roll(e[g * per + j, own_r, own_c], (lax.rem(j + 1, per)) * width, 1)
            r, l = carry[i]
            done.append((jnp.where(at_right, t, r), jnp.where(at_left, t, l)))
        return tuple(done)

    zero = jnp.zeros((rows, lanes), jnp.float32)
    packed = loop(per, pack, tuple((zero, zero) for _ in range(4 * groups)), PACK)
    for i, (r, l) in enumerate(packed):
        to_right[i] = r
        to_left[i] = l

    lefts_there = (gy + ny_parts - 1) // ny_parts
    rights_there = (2 * ny_parts - 2 - gy) // ny_parts
    pl.semaphore_wait(barrier, 2 + 2 * lefts_there + 2 * rights_there)

    def remote(src, dst, send, recv, device):
        return pltpu.make_async_remote_copy(
            src_ref=src, dst_ref=dst, send_sem=send, recv_sem=recv,
            device_id=device, device_id_type=pl.DeviceIdType.MESH,
        )

    lefts = [
        remote(to_left, from_right.at[t], ys_sem.at[t], yr_sem.at[t], left[t]) for t in range(2)
    ]
    rights = [
        remote(to_right, from_left.at[t], ys_sem.at[2 + t], yr_sem.at[2 + t], right[t])
        for t in range(2)
    ]

    @pl.when(has_left)
    def _():
        for c in lefts:
            c.start()

    @pl.when(has_right)
    def _():
        for c in rights:
            c.start()

    xs = [
        remote(
            e.at[:, own_r, own_c], e.at[:, other_r, own_c], xs_sem.at[a], xr_sem.at[a], x_peer
        )
        for a, e in enumerate(exts)
    ]
    for a in (2, 0, 1, 3):
        xs[a].start()

    def layer(k):
        return k + gz * (n - 1 - 2 * k)

    def shift(h):
        return table[index[h]]

    def inverse(h, shape):
        return 1.0 / jnp.full(shape, shift(h), jnp.float32)

    def factor(r_at, c_at, hs):
        shape = (r_at.size, lanes)
        inv = inverse_all(hs, shape)
        one = jnp.ones(shape, jnp.float32)

        def body(k, carry):
            z = layer(k)
            rl = 1.0 / lc_x[z, r_at, c_at]
            pc, src = pc_x[z, r_at, c_at], src_x[z, r_at, c_at]
            four = 4.0 * pc
            done = []
            for (p, d), h, i in zip(carry, hs, inv):
                d = d + (rl * i) * p
                q = p + d
                p_s[h, z, r_at, c_at] = p
                pr = p * rl
                own_s[h, z, r_at, c_at] = pr * (i - four)
                near_s[h, z, r_at, c_at] = pr * pc
                src_s[h, z, r_at, c_at] = pr * src
                b_s[h, z, r_at, c_at] = 1.0 / (p * q)
                done.append((q, d))
            return tuple(done)

        final = loop(n, body, tuple((one, one) for _ in hs), FACTOR)
        for (q, d), h in zip(final, hs):
            iq = 1.0 / q
            iq_s[h, r_at, c_at] = iq
            beta_s[h, r_at, c_at] = d * iq

    def inverse_all(hs, shape):
        return [inverse(h, shape) for h in hs]

    steps = list(range(half))
    factor(own_r, own_c, steps)
    for a in (2, 0, 1, 3):
        xs[a].wait()
    factor(other_r, own_c, steps[:-1])

    def send_beta(h, c_at, i):
        return remote(
            beta_s.at[h, :, c_at], beta_r.at[h, :, c_at], bs_sem.at[i], br_sem.at[i], z_peer
        )

    last = half - 1
    betas = [[send_beta(h, own_c, h)] for h in steps[:-1]]
    betas.append(
        [remote(
            beta_s.at[last, own_r, own_c], beta_r.at[last, own_r, own_c],
            bs_sem.at[last], br_sem.at[last], z_peer,
        )]
    )
    for b in betas:
        b[0].start()

    @pl.when(has_left)
    def _():
        for c in lefts:
            c.wait_send()
        for c in rights:
            c.wait_recv()

    @pl.when(has_right)
    def _():
        for c in rights:
            c.wait_send()
        for c in lefts:
            c.wait_recv()

    inside = ((lane < width) & has_right) | ((lane >= lanes - width) & has_left)

    filler = lc_x[0, own_r, own_c]

    def unpack(j, carry):
        at_left = slot(lax.rem(j + 1, per))
        back = (per - 1 - j) * width
        for t in range(2):
            r_at = pl.ds(t * rows, rows)
            for a, e in enumerate(exts):
                for g in range(groups):
                    i = a * groups + g
                    both = jnp.where(at_left, from_right[t, i], from_left[t, i])
                    z = g * per + j
                    rest = filler if a == 2 else zero
                    e[z, r_at, halo_c] = jnp.where(inside, pltpu.roll(both, back, 1), rest)
        return carry

    loop(per, unpack, 0, UNPACK)

    def factor_halo(h):
        factor(all_r, halo_c, [h])
        c = send_beta(h, halo_c, half + h)
        c.start()
        betas[h].append(c)

    factor_halo(0)

    wide = (2 * rows, 2 * lanes)
    row = lax.broadcasted_iota(jnp.int32, wide, 0)
    top = row == gx * rows
    bottom = row == (2 * rows - 1 + gx * rows) % (2 * rows)

    def edges(u):
        return (
            jnp.where(top, 0.0, pltpu.roll(u, 1, 0))
            + jnp.where(bottom, 0.0, pltpu.roll(u, 2 * rows - 1, 0))
            + pltpu.roll(u, 1, 1)
            + pltpu.roll(u, 2 * lanes - 1, 1)
        )

    def explicit(h, field):
        r_at, c_at, shape, cut = part(h)

        def body(k, total):
            z = layer(k)
            u = field(z)
            beside = cut(edges(u))
            g = own_s[h, z, r_at, c_at] * cut(u) + (
                near_s[h, z, r_at, c_at] * beside + src_s[h, z, r_at, c_at]
            )
            g_s[z, r_at, c_at] = g
            return total + g

        return loop(n, body, jnp.zeros(shape, jnp.float32), EXPLICIT)

    def part(h):
        if h == last:
            return own_r, own_c, (rows, lanes), lambda a: a[:rows, :lanes]
        return all_r, pl.ds(0, 2 * lanes), wide, lambda a: a

    total = explicit(0, lambda z: u_x[z])
    for h in steps:
        r_at, c_at, shape, _ = part(h)
        iq = iq_s[h, r_at, c_at]
        face = total * iq
        face_s[h, r_at, c_at] = face
        send = remote(
            face_s.at[h, r_at, c_at], face_r.at[h, r_at, c_at], fs_sem.at[h], fr_sem.at[h], z_peer
        )
        send.start()
        zero_part = jnp.zeros(shape, jnp.float32)

        def ahead(k, total, h=h, r_at=r_at, c_at=c_at):
            z = layer(k)
            total = total + g_s[z, r_at, c_at]
            f_s[z, r_at, c_at] = total * b_s[h, z, r_at, c_at]
            return total

        def behind(k, total, h=h, r_at=r_at, c_at=c_at):
            z = layer(k)
            total = total + f_s[z, r_at, c_at]
            w_s[z, r_at, c_at] = p_s[h, z, r_at, c_at] * total
            return total

        loop(n, ahead, zero_part, SUMS)
        loop(n, behind, zero_part, SUMS, reverse=True)
        if h + 1 < last:
            factor_halo(h + 1)
        for b in betas[h]:
            b.wait()
        mine, theirs = beta_s[h, r_at, c_at], beta_r[h, r_at, c_at]
        gain = iq / (mine + theirs - mine * theirs)
        partial = (1.0 - theirs) * face
        send.wait()
        v = (face_r[h, r_at, c_at] + partial) * gain

        def solved(z, h=h, v=v, r_at=r_at, c_at=c_at):
            return p_s[h, z, r_at, c_at] * v + w_s[z, r_at, c_at]

        if h < last:
            total = explicit(h + 1, solved)
        else:

            def write(z, carry):
                out[z] = solved(z)
                return carry

            loop(n, write, 0, SUMS)


def solution(mesh):
    ny_parts = mesh.shape["gy"]
    assert mesh.shape["gz"] == 2 and mesh.shape["gx"] == 2

    def on_device(u, pc, lc, src, table, index):
        half = index.shape[0]
        n, rows, lanes = u.shape
        f32 = jnp.float32
        ext = pltpu.VMEM((n, 2 * rows, 2 * lanes), f32)
        coef = pltpu.VMEM((half, n, 2 * rows, 2 * lanes), f32)
        face = pltpu.VMEM((half, 2 * rows, 2 * lanes), f32)
        count = 4 * (n * half // lanes)
        pack = pltpu.VMEM((count, rows, lanes), f32)
        packs = pltpu.VMEM((2, count, rows, lanes), f32)
        dma = pltpu.SemaphoreType.DMA
        return pl.pallas_call(
            functools.partial(kernel, ny_parts, half),
            out_shape=pltpu.VMEM(u.shape, f32),
            in_specs=[pl.BlockSpec(memory_space=pl.ANY)] * 4
            + [pl.BlockSpec(memory_space=pltpu.SMEM)] * 2,
            out_specs=pl.BlockSpec(memory_space=pltpu.VMEM),
            scratch_shapes=[ext] * 4 + [pack] * 2 + [packs] * 2
            + [coef] * 5 + [ext] * 3 + [face] * 5
            + [dma((4,)), dma((4,)), dma((4,)), dma((4,)), dma((4,)),
               dma((2 * half,)), dma((2 * half,)), dma((half,)), dma((half,))],
            compiler_params=pltpu.CompilerParams(collective_id=0, has_side_effects=True),
        )(u, pc, lc, src, table, index)

    spec = P("gz", "gx", "gy")
    return jax.shard_map(
        on_device, mesh=mesh, in_specs=(spec,) * 4 + (P(), P()), out_specs=spec, check_vma=False
    )
```
